256 devices in a mesh: dp: 64 (over z, x, core), tensor: 4 (over y).
Axes of the slice: x: 4, y: 4, z: 8, core: 2. Of those that a mesh axis runs over, the one named last changes fastest.
Arguments:
- grads: bfloat16 [64, 160, 28672], P('dp', None, 'tensor'), may hold values from -336000 to 336000, as said below
- error: bfloat16 [64, 160, 28672], P('dp', None, 'tensor'), may hold values from -0.8984375 to 0.8984375
- q_init: float32 [28672, 64], P('tensor'), may hold values from -6 to 6
Outputs:
- p_factor: float32 [160, 64], replicated
- q_factor: float32 [28672, 64], P('tensor')
- new_error: float32 [64, 160, 28672], P('dp', None, 'tensor')
The draws below stay inside these ranges and needn't reach their ends.
Inputs may be any that keep to these rules, and one draw needn't show every extreme that they name: `grads`: entries of the gradients; each replica's gradient has its own overall scale.
All inputs are finite; a program needn't handle non-finite values.
Results may differ from the reference program's by a relative error of at most 0.0025.
The reference program's roundings to bfloat16 on the way (of `q_half` and `p_half`) count: a program that leaves them out, or rounds other values in their place, can miss the bound.
Values may be sent and summed in bfloat16 or wider, within the bound.
No kernel may reach another device: no remote copies, remote signals or barrier semaphores. Data moves between devices by JAX's collectives and lax.ppermute only.
A program may use at most 64 MiB of HBM per device.

```python
import math
import jax
import jax.numpy as jnp
from jax import lax

ROWS = 160
COLS = 28672
RANK = 64
ITERS = 2
N_DP = 64


def draw_grads(key, part):
    keys = jax.random.split(jax.random.fold_in(key, 17), 3)
    noise = jnp.clip(jax.random.normal(keys[0], (N_DP, ROWS, COLS), jnp.float32), -4.0, 4.0)
    row_scale = jnp.exp(jax.random.uniform(keys[1], (1, ROWS, 1), jnp.float32) * math.log(10.0))
    col_scale = jnp.exp(jax.random.uniform(keys[2], (1, 1, COLS), jnp.float32) * math.log(10.0))
    ladder = jnp.arange(N_DP, dtype=jnp.float32) / max(N_DP - 1, 1)
    replica_scale = 200.0 ** ladder
    return (noise * row_scale * col_scale * replica_scale[:, None, None]).astype(jnp.bfloat16)


def levels(key, extent, cuts, low, top_value):
    def one(dim, parts):
        heights = jax.random.uniform(jax.random.fold_in(jax.random.fold_in(key, 6), dim), (parts,), jnp.float32, low / len(cuts), top_value / len(cuts))
        return jnp.repeat(jnp.exp(heights), extent[dim] // parts).reshape((-1,) + (1,) * (len(extent) - dim - 1))

    level = one(*cuts[0])
    for cut in cuts[1:]:
        level = level * one(*cut)
    return level


def centred(stream_key, shape, width, bound, cuts=(), kind=jnp.bfloat16):
    factor_of = levels(stream_key, shape, cuts, -0.22, 0.18) if cuts else 1.0
    result = jax.random.normal(stream_key, shape, jnp.float32) * width * factor_of
    return jnp.minimum(jnp.maximum(result, -bound), bound).astype(kind)


def setup_inputs(seed: int = 0) -> dict:
    arg_keys = jax.random.split(jax.random.key(seed), 4)
    grads = draw_grads(jax.random.fold_in(arg_keys[3], 71), 0)
    error = centred(arg_keys[1], (N_DP, ROWS, COLS), 0.15, 0.8984375, ((0, 64), (2, 4)))
    q_init = centred(arg_keys[2], (COLS, RANK), 1.0, 6.0, ((0, 4),), jnp.float32)
    return dict(grads=grads, error=error, q_init=q_init)


epsilon = 1e-06
clip_ratio = 0.5

def orthonormal(matrix):
    rank_width = matrix.shape[1]
    columns = lax.broadcasted_iota(jnp.int32, (1, rank_width), 1)

    def sweep_col(position, vectors):
        position = position.astype(jnp.int32)
        column = lax.dynamic_slice_in_dim(vectors, position, 1, 1)
        column = column * lax.rsqrt(jnp.sum(column * column) + epsilon)
        vectors = lax.dynamic_update_slice_in_dim(vectors, column, position, 1)
        coeffs = jnp.dot(column.T, vectors, precision=lax.Precision.HIGHEST)
        coeffs = jnp.where(columns > position, coeffs, jnp.zeros_like(coeffs))
        return vectors - jnp.dot(column, coeffs, precision=lax.Precision.HIGHEST)
    return lax.fori_loop(jnp.int32(0), jnp.int32(rank_width), sweep_col, matrix)

def reference(grads, error, q_init):

    def add_squares(carry, gradient):
        return (carry + jnp.sum(jnp.square(gradient.astype(jnp.float32))), None)
    sum_squares, unused = lax.scan(add_squares, jnp.zeros((), jnp.float32), grads)
    shrink = jnp.minimum(1.0, clip_ratio * jnp.sqrt(jnp.float32(ROWS * COLS)) * lax.rsqrt(sum_squares / N_DP + epsilon))

    def merge(gradient, residue):
        return shrink * gradient.astype(jnp.float32) + residue.astype(jnp.float32)
    q_full = q_init
    p_hat = jnp.zeros((ROWS, RANK), jnp.float32)
    for sweep in range(ITERS):
        q_wide = q_full.astype(jnp.bfloat16).astype(jnp.float32)

        def left_step(carry, pieces):
            merged = merge(pieces[0], pieces[1])
            return (carry + jnp.dot(merged, q_wide, precision=lax.Precision.HIGHEST), None)
        p_sum, unused = lax.scan(left_step, jnp.zeros((ROWS, RANK), jnp.float32), (grads, error))
        p_hat = orthonormal(p_sum)
        p_wide = p_hat.astype(jnp.bfloat16).astype(jnp.float32)

        def right_step(carry, pieces):
            merged = merge(pieces[0], pieces[1])
            return (carry + jnp.dot(merged.T, p_wide, precision=lax.Precision.HIGHEST), None)
        q_sum, unused = lax.scan(right_step, jnp.zeros((COLS, RANK), jnp.float32), (grads, error))
        q_full = q_sum / N_DP
    p_half = p_hat.astype(jnp.bfloat16)
    q_half = q_full.astype(jnp.bfloat16)
    approx = jnp.dot(p_half, q_half.T, preferred_element_type=jnp.float32)

    def fresh_error(pieces):
        return merge(pieces[0], pieces[1]) - approx
    new_error = lax.map(fresh_error, (grads, error))
    return (p_hat, q_full, new_error)
```

```python
import functools

import jax
import jax.numpy as jnp
from jax import lax
from jax.experimental import pallas as pl
from jax.experimental.pallas import tpu as pltpu
from jax.sharding import Mesh
from jax.sharding import PartitionSpec as P

ROWS = 160
COLS = 28672
RANK = 64
LOCAL = 7168
HALF = LOCAL // 2
QUARTER = HALF // 4
LANES = 128
BLOCKS = QUARTER // LANES
TAIL = ROWS - LANES
REPLICAS = 64
EPS = 1e-06
CLIP = 0.5

f32 = jnp.float32
bf16 = jnp.bfloat16
HIGHEST = lax.Precision.HIGHEST
VMEM = pltpu.VMEM


def whole():
    return pl.BlockSpec(memory_space=VMEM)


def shrink_of(squares):
    rows = jnp.sum(squares, axis=0)
    total = jnp.sum(jnp.sum(rows, axis=1, keepdims=True), axis=0, keepdims=True)
    scaled = CLIP * jnp.sqrt(f32(ROWS * COLS))
    return jnp.minimum(1.0, scaled * lax.rsqrt(total / REPLICAS + EPS))


def prep_kernel(at, g, e, send, squares):
    step = pl.program_id(0)

    @pl.when(step == 0)
    def _():
        squares[...] = jnp.zeros_like(squares)

    def rows(i, total):
        block = g[0, pl.ds(i * 16, 16), :].astype(f32)
        block = block * block
        part = block[:8] + block[8:]
        for lane in range(0, part.shape[1], LANES):
            total = total + part[:, lane : lane + LANES]
        return total

    squares[...] += lax.fori_loop(0, ROWS // 16, rows, jnp.zeros((8, LANES), f32))

    @pl.when(step < 2)
    def _():
        send[0:ROWS, :] = g[0]
        send[ROWS:, :] = e[0]


def prep(at, grads, error):
    width = HALF // 2
    mine = lambda i, at: (0, 0, jnp.where(i < 2, (1 - at[0]) * 2 + i, at[0] * 2 + i - 2))
    theirs = lambda i, at: (0, 0, (1 - at[0]) * 2 + jnp.minimum(i, 1))
    return pl.pallas_call(
        prep_kernel,
        grid_spec=pltpu.PrefetchScalarGridSpec(
            num_scalar_prefetch=1,
            grid=(4,),
            in_specs=[pl.BlockSpec((1, ROWS, width), mine), pl.BlockSpec((1, ROWS, width), theirs)],
            out_specs=[
                pl.BlockSpec((2 * ROWS, width), lambda i, at: (0, jnp.minimum(i, 1))),
                pl.BlockSpec((8, LANES), lambda i, at: (0, 0)),
            ],
        ),
        out_shape=[
            jax.ShapeDtypeStruct((2 * ROWS, HALF), bf16),
            jax.ShapeDtypeStruct((8, LANES), f32),
        ],
        name="prep",
    )(at, grads, error)


def merge_kernel(at, g, e, got, squares, *outs):
    shrink = shrink_of(squares[...])
    for j, out in enumerate(outs):
        first = pl.multiple_of(lax.rem(at[1] + j, 4) * QUARTER, LANES)

        def rows(i, carry, out=out, first=first):
            here, cols = pl.ds(i * 16, 16), pl.ds(first, QUARTER)
            gradient = g[0, here, cols].astype(f32) + got[here, cols].astype(f32)
            residue = e[0, here, cols].astype(f32) + got[pl.ds(ROWS + i * 16, 16), cols].astype(f32)
            out[here, :] = shrink * gradient + residue
            return carry

        lax.fori_loop(0, ROWS // 16, rows, 0)


def merge(at, grads, error, got, squares):
    own = pl.BlockSpec((1, ROWS, HALF), lambda i, at: (0, 0, at[0]))
    return pl.pallas_call(
        merge_kernel,
        grid_spec=pltpu.PrefetchScalarGridSpec(
            num_scalar_prefetch=1,
            grid=(1,),
            in_specs=[
                own,
                own,
                pl.BlockSpec((2 * ROWS, HALF), lambda i, at: (0, 0)),
                pl.BlockSpec((8, 8, LANES), lambda i, at: (0, 0, 0)),
            ],
            out_specs=[pl.BlockSpec((ROWS, QUARTER), lambda i, at: (0, 0))] * 4,
        ),
        out_shape=[jax.ShapeDtypeStruct((ROWS, QUARTER), f32)] * 4,
        name="merge",
    )(at, grads, error, got, squares)


def fold_kernel(a, b, c, d, out):
    for k in range(BLOCKS):
        cols = slice(k * LANES, (k + 1) * LANES)
        out[k] = (a[:, cols] + c[:, cols]) + (b[:, cols] + d[:, cols])
    out[BLOCKS] = jnp.zeros((ROWS, LANES), f32)


def fold(parts):
    return pl.pallas_call(
        fold_kernel,
        in_specs=[whole()] * 4,
        out_specs=whole(),
        out_shape=jax.ShapeDtypeStruct((BLOCKS + 1, ROWS, LANES), f32),
        name="fold",
    )(*parts)


def dot(a, b):
    return jnp.dot(a, b, precision=HIGHEST, preferred_element_type=f32)


def dot_t(a, b):
    return lax.dot_general(
        a, b, (((1,), (1,)), ((), ())), precision=HIGHEST, preferred_element_type=f32
    )


def terms_kernel(at, pieces, q, total, pack):
    s = pieces[0]
    for k in range(1, BLOCKS + 1):
        s = s + pieces[k]
    total[...] = s
    head = s[:LANES]
    tail = s[LANES:]
    tail_full = jnp.concatenate([tail, jnp.zeros((LANES - TAIL, LANES), f32)], axis=0)
    q_half = q[...].astype(bf16).astype(f32)
    left_tail = dot_t(q_half, tail_full)
    corner = dot_t(tail, tail_full)
    packed_left = left_tail[0:16]
    packed_corner = corner[0:8]
    for j in range(1, 4):
        packed_left = packed_left + pltpu.roll(left_tail[16 * j : 16 * j + 16], 32 * j, 1)
        packed_corner = packed_corner + pltpu.roll(corner[8 * j : 8 * j + 8], 32 * j, 1)
    flat = jnp.concatenate(
        [
            dot_t(q_half, head),
            dot_t(head, head),
            dot_t(tail, head),
            packed_left,
            packed_corner,
            jnp.zeros((8, LANES), f32),
        ],
        axis=0,
    )
    for k in range(8):
        pack[k] = flat[32 * k : 32 * k + 32]


def terms(at, pieces, q_t):
    column = lambda i, at: (0, at[0] * 4 * BLOCKS + at[1] * BLOCKS + jnp.minimum(at[2], BLOCKS - 1))
    return pl.pallas_call(
        terms_kernel,
        grid_spec=pltpu.PrefetchScalarGridSpec(
            num_scalar_prefetch=1,
            grid=(1,),
            in_specs=[
                pl.BlockSpec((BLOCKS + 1, ROWS, LANES), lambda i, at: (0, 0, 0)),
                pl.BlockSpec((RANK, LANES), column),
            ],
            out_specs=[
                pl.BlockSpec((ROWS, LANES), lambda i, at: (0, 0)),
                pl.BlockSpec((8, 32, LANES), lambda i, at: (0, 0, 0)),
            ],
        ),
        out_shape=[
            jax.ShapeDtypeStruct((ROWS, LANES), f32),
            jax.ShapeDtypeStruct((8, 32, LANES), f32),
        ],
        name="terms",
    )(at, pieces, q_t)


def orthonormal(a, b):
    groups = RANK // 8
    a = [a[8 * i : 8 * i + 8] for i in range(groups)]
    b = [b[8 * i : 8 * i + 8] for i in range(groups)]
    place = lax.broadcasted_iota(jnp.int32, (8, 1), 0)
    for k in range(RANK):
        g, r = divmod(k, 8)
        row_a, row_b = a[g][r : r + 1], b[g][r : r + 1]
        dots = [
            jnp.sum(a[i] * row_a + b[i] * row_b, axis=1, keepdims=True) for i in range(g, groups)
        ]
        inverse = 1.0 / (dots[0][r : r + 1] + EPS)
        for i in range(g, groups):
            coeff = dots[i - g] * inverse
            if i == g:
                coeff = jnp.where(place > r, coeff, 0.0)
            a[i] = a[i] - coeff * row_a
            b[i] = b[i] - coeff * row_b
    for i in range(groups):
        scale = lax.rsqrt(jnp.sum(a[i] * a[i] + b[i] * b[i], axis=1, keepdims=True) + EPS)
        a[i] = a[i] * scale
        b[i] = b[i] * scale
    return jnp.concatenate(a, axis=0), jnp.concatenate(b, axis=0)


def factor_kernel(pack, s, p_t, p_half, q):
    lane = lax.broadcasted_iota(jnp.int32, (1, LANES), 1)
    keep = lane < TAIL

    def unpack(rows):
        parts = [jnp.where(keep, rows, 0.0)]
        for j in range(1, 4):
            parts.append(jnp.where(keep, pltpu.roll(rows, LANES - 32 * j, 1), 0.0))
        return jnp.concatenate(parts, axis=0)

    flat = jnp.concatenate([pack[k] for k in range(8)], axis=0)
    empty = jnp.zeros((LANES - TAIL, LANES), f32)
    first_a = flat[0:64]
    gram = flat[64 : 64 + LANES]
    gram_side = jnp.concatenate([flat[64 + LANES : 64 + ROWS], empty], axis=0)
    first_b = unpack(flat[224:240])
    gram_corner = jnp.concatenate([unpack(flat[240:248]), empty], axis=0)

    a, b = orthonormal(first_a, first_b)
    a = a.astype(bf16).astype(f32)
    b = b.astype(bf16).astype(f32)
    second_a = (dot(a, gram) + dot(b, gram_side)) * (1.0 / REPLICAS)
    second_b = (dot_t(a, gram_side) + dot(b, gram_corner)) * (1.0 / REPLICAS)
    a, b = orthonormal(second_a, second_b)
    p_t[:, 0:LANES] = a
    p_t[:, LANES:ROWS] = b[:, 0:TAIL]
    a = a.astype(bf16).astype(f32)
    b = b.astype(bf16).astype(f32)
    p_half[0:LANES, :] = a.T.astype(bf16)
    p_half[LANES:ROWS, :] = b.T[0:TAIL].astype(bf16)
    tail_full = jnp.concatenate([s[LANES:ROWS], empty], axis=0)
    q[...] = ((dot(a, s[0:LANES]) + dot(b, tail_full)) * (1.0 / REPLICAS)).astype(q.dtype)


def factor(pack, s):
    return pl.pallas_call(
        factor_kernel,
        in_specs=[whole()] * 2,
        out_specs=[whole()] * 3,
        out_shape=[
            jax.ShapeDtypeStruct((RANK, ROWS), f32),
            jax.ShapeDtypeStruct((ROWS, RANK), bf16),
            jax.ShapeDtypeStruct((RANK, LANES), bf16),
        ],
        name="factor",
    )(pack, s)


def finish_kernel(at, g, e, squares, p_half, *refs):
    parts, (out, q_t) = refs[:8], refs[8:]
    shrink = shrink_of(squares[...])
    for k in range(8):

        @pl.when(pl.program_id(0) == k)
        def _(part=parts[k]):
            for block in range(BLOCKS):
                cols = slice(block * LANES, (block + 1) * LANES)
                q = part[block]
                approx = jnp.dot(p_half[...], q, preferred_element_type=f32)
                merged = shrink * g[0, :, cols].astype(f32) + e[0, :, cols].astype(f32)
                out[0, :, cols] = merged - approx
                q_t[:, cols] = q.astype(f32)


def finish(at, grads, error, squares, p_half, parts):
    def column(i, at):
        core = jnp.where(i < 4, at[0], 1 - at[0])
        return core * 4 + lax.rem(at[1] + i, 4)

    tile = pl.BlockSpec((1, ROWS, QUARTER), lambda i, at: (0, 0, column(i, at)))
    return pl.pallas_call(
        finish_kernel,
        grid_spec=pltpu.PrefetchScalarGridSpec(
            num_scalar_prefetch=1,
            grid=(8,),
            in_specs=[
                tile,
                tile,
                pl.BlockSpec((8, 8, LANES), lambda i, at: (0, 0, 0)),
                pl.BlockSpec((ROWS, RANK), lambda i, at: (0, 0)),
            ]
            + [pl.BlockSpec((8, RANK, LANES), lambda i, at: (0, 0, 0))] * 8,
            out_specs=[tile, pl.BlockSpec((RANK, QUARTER), lambda i, at: (0, column(i, at)))],
        ),
        out_shape=[
            jax.ShapeDtypeStruct((1, ROWS, LOCAL), f32),
            jax.ShapeDtypeStruct((RANK, LOCAL), f32),
        ],
        name="finish",
    )(at, grads, error, squares, p_half, *parts)


def shifted(value, axis, by):
    n = lax.axis_size(axis)
    return lax.ppermute(value, axis, [(i, (i - by) % n) for i in range(n)])


def swap(value, axis):
    return lax.ppermute(value, axis, [(0, 1), (1, 0)])


def from_ring(value, axis):
    return [value] + [shifted(value, axis, j) for j in range(1, 4)]


def ring_sum(value, axis):
    a, b, c, d = from_ring(value, axis)
    return (a + c) + (b + d)


def exchange(blocks, axis):
    return lax.all_to_all(blocks, axis, 0, 0, tiled=True)


def everyone(value, axis, n):
    return exchange(jnp.broadcast_to(value[None], (n, *value.shape)), axis)


def local(grads, error, q_init):
    at = jnp.stack([lax.axis_index("c"), lax.axis_index("x"), lax.axis_index("z")]).astype(jnp.int32)
    send, squares = prep(at, grads, error)
    got = swap(send, "c")
    squares = squares + swap(squares, "c")
    squares = ring_sum(ring_sum(squares, "x"), "y")
    squares = everyone(squares, "z", 8)

    pieces = merge(at, grads, error, got, squares)
    pieces = [pieces[0]] + [shifted(pieces[j], "x", -j) for j in range(1, 4)]
    pieces = exchange(fold(pieces), "z")
    s, pack = terms(at, pieces, q_init.T)

    piece = jnp.sum(exchange(pack, ("c", "y")), axis=0)
    piece = ring_sum(piece, "x")
    piece = jnp.sum(everyone(piece, "z", 8), axis=0)
    pack = everyone(piece, ("c", "y"), 8)

    p_t, p_half, q = factor(pack, s)
    parts = from_ring(everyone(q, "z", 8), "x")
    parts = parts + [swap(part, "c") for part in parts]
    new_error, q_t = finish(at, grads, error, squares, p_half, parts)
    return p_t.T, q_t.T, new_error


def solution(mesh):
    finer = Mesh(
        mesh.devices.reshape(8, 4, 2, mesh.shape["tensor"]), ("z", "x", "c", "y")
    )
    replicas = ("z", "x", "c")
    return jax.shard_map(
        local,
        mesh=finer,
        in_specs=(P(replicas, None, "y"), P(replicas, None, "y"), P("y", None)),
        out_specs=(P(), P("y", None), P(replicas, None, "y")),
        check_vma=False,
    )
```

```python
import functools

import jax
import jax.numpy as jnp
from jax import lax
from jax.experimental import pallas as pl
from jax.experimental.pallas import tpu as pltpu
from jax.sharding import Mesh
from jax.sharding import PartitionSpec as P


ROWS = 160
COLS = 28672
RANK = 64
LOCAL = 7168
HALF = LOCAL // 2
QUARTER = HALF // 4
LANES = 128
BLOCKS = QUARTER // LANES
TAIL = ROWS - LANES
EARLY = 48
LATE = ROWS - EARLY
SPREAD = 32
REPLICAS = 64
EPS = 1e-06
CLIP = 0.5

f32 = jnp.float32
bf16 = jnp.bfloat16
HIGHEST = lax.Precision.HIGHEST
VMEM = pltpu.VMEM


def whole():
    return pl.BlockSpec(memory_space=VMEM)


def room(mib, flops=10**6):
    return dict(
        compiler_params=pltpu.CompilerParams(vmem_limit_bytes=mib * 2**20),
        cost_estimate=pl.CostEstimate(flops=flops, bytes_accessed=2**20, transcendentals=0),
    )


def shrink_of(squares):
    rows = jnp.sum(squares, axis=0)
    total = jnp.sum(jnp.sum(rows, axis=1, keepdims=True), axis=0, keepdims=True)
    scaled = CLIP * jnp.sqrt(f32(ROWS * COLS))
    return jnp.minimum(1.0, scaled * lax.rsqrt(total / REPLICAS + EPS))


def prep_kernel(at, g, e, q_all, send, squares, q, own, sems):
    def piece(ref, core, out, sem):
        cols = pl.ds(pl.multiple_of(core * HALF, LANES), HALF)
        return pltpu.make_async_copy(ref.at[0, :, cols], out, sems.at[sem])

    copies = [
        piece(g, 1 - at[0], send.at[0:ROWS], 0),
        piece(g, at[0], own, 1),
        piece(e, 1 - at[0], send.at[ROWS : 2 * ROWS], 2),
    ]
    first = at[0] * 4 * BLOCKS + at[1] * BLOCKS + jnp.minimum(at[2], BLOCKS - 1)
    cols = pl.ds(pl.multiple_of(first * LANES, LANES), LANES)
    copies.append(pltpu.make_async_copy(q_all.at[:, cols], q, sems.at[3]))
    for copy in copies:
        copy.start()

    def rows_of(ref):
        def rows(i, acc):
            for lane in range(0, HALF, HALF // 4):
                block = ref[pl.ds(i * 16, 16), lane : lane + HALF // 4].astype(f32)
                block = block * block
                acc = acc + (block[:8] + block[8:])
            return acc

        return rows

    acc = jnp.zeros((8, HALF // 4), f32)
    copies[0].wait()
    acc = lax.fori_loop(0, ROWS // 16, rows_of(send), acc)
    copies[1].wait()
    acc = lax.fori_loop(0, ROWS // 16, rows_of(own), acc)
    part = acc[:, :LANES]
    for lane in range(LANES, HALF // 4, LANES):
        part = part + acc[:, lane : lane + LANES]
    for k in range(SPREAD):
        squares[k] = part
    copies[2].wait()
    copies[3].wait()


def prep(at, grads, error, q_t):
    hbm = pl.BlockSpec(memory_space=pltpu.HBM)
    return pl.pallas_call(
        prep_kernel,
        grid_spec=pltpu.PrefetchScalarGridSpec(
            num_scalar_prefetch=1,
            grid=(1,),
            in_specs=[hbm, hbm, hbm],
            out_specs=[
                pl.BlockSpec((2 * ROWS, HALF), lambda i, at: (0, 0)),
                pl.BlockSpec((SPREAD, 8, LANES), lambda i, at: (0, 0, 0)),
                pl.BlockSpec((RANK, LANES), lambda i, at: (0, 0)),
            ],
            scratch_shapes=[VMEM((ROWS, HALF), bf16), pltpu.SemaphoreType.DMA((4,))],
        ),
        out_shape=[
            jax.ShapeDtypeStruct((2 * ROWS, HALF), bf16),
            jax.ShapeDtypeStruct((SPREAD, 8, LANES), f32),
            jax.ShapeDtypeStruct((RANK, LANES), f32),
        ],
        name="prep",
        **room(58, 10**8),
    )(at, grads, error, q_t)


def both(g, e, got, row, cols):
    here = pl.ds(row, 16)
    gradient = g[0, here, cols].astype(f32) + got[here, cols].astype(f32)
    residue = e[0, here, cols].astype(f32) + got[pl.ds(ROWS + row, 16), cols].astype(f32)
    return gradient, residue


def early_kernel(at, g, e, got, squares, *outs):
    outs, spread = outs[:4], outs[4]
    for j, out in enumerate(outs):
        cols = pl.ds(pl.multiple_of(lax.rem(at[1] + j, 4) * QUARTER, LANES), QUARTER)

        def rows(i, carry, out=out, cols=cols):
            gradient, residue = both(g, e, got, i * 16, cols)
            out[pl.ds(i * 16, 16), :] = gradient
            out[pl.ds(EARLY + i * 16, 16), :] = residue
            return carry

        lax.fori_loop(0, EARLY // 16, rows, 0)
    total = jnp.sum(squares[...], axis=0)
    for k in range(8):
        spread[k] = total


def late_kernel(at, g, e, got, squares, *outs):
    outs, spread = outs[:4], outs[4]
    shrink = shrink_of(squares[...])
    spread[...] = jnp.broadcast_to(shrink, (8, LANES))
    for j, out in enumerate(outs):
        cols = pl.ds(pl.multiple_of(lax.rem(at[1] + j, 4) * QUARTER, LANES), QUARTER)

        def rows(i, carry, out=out, cols=cols):
            gradient, residue = both(g, e, got, EARLY + i * 16, cols)
            out[pl.ds(i * 16, 16), :] = shrink * gradient + residue
            return carry

        lax.fori_loop(0, LATE // 16, rows, 0)


def merge(kernel, at, grads, error, got, squares, rows, spread):
    own = pl.BlockSpec((1, ROWS, HALF), lambda i, at: (0, 0, at[0]))
    outs = [((rows, QUARTER), f32)] * 4
    outs = outs + [((*spread, 8, LANES), f32)]
    return pl.pallas_call(
        kernel,
        grid_spec=pltpu.PrefetchScalarGridSpec(
            num_scalar_prefetch=1,
            grid=(1,),
            in_specs=[
                own,
                own,
                pl.BlockSpec((2 * ROWS, HALF), lambda i, at: (0, 0)),
                pl.BlockSpec(squares.shape, lambda i, at: (0, 0, 0)),
            ],
            out_specs=[
                pl.BlockSpec(shape, lambda i, at, shape=shape: (0,) * len(shape))
                for shape, _ in outs
            ],
        ),
        out_shape=[jax.ShapeDtypeStruct(*out) for out in outs],
        **room(16, 10**9),
    )(at, grads, error, got, squares)


def fold_early_kernel(a, b, c, d, shrink, out):
    shrink = shrink[0:1, 0:1]
    top, low = slice(0, EARLY), slice(EARLY, 2 * EARLY)
    for k in range(BLOCKS):
        cols = slice(k * LANES, (k + 1) * LANES)
        gradient = (a[top, cols] + c[top, cols]) + (b[top, cols] + d[top, cols])
        residue = (a[low, cols] + c[low, cols]) + (b[low, cols] + d[low, cols])
        out[k] = shrink * gradient + residue
    out[BLOCKS] = jnp.zeros((EARLY, LANES), f32)


def fold_late_kernel(a, b, c, d, after, out):
    for k in range(BLOCKS):
        cols = slice(k * LANES, (k + 1) * LANES)
        out[k] = (a[:, cols] + c[:, cols]) + (b[:, cols] + d[:, cols])
    out[BLOCKS] = jnp.zeros((LATE, LANES), f32)


def fold(kernel, rows, *args):
    return pl.pallas_call(
        kernel,
        in_specs=[whole()] * len(args),
        out_specs=whole(),
        out_shape=jax.ShapeDtypeStruct((BLOCKS + 1, rows, LANES), f32),
        **room(8, 10**8),
    )(*args)


def dot(a, b):
    return jnp.dot(a, b, precision=HIGHEST, preferred_element_type=f32)


def dot_t(a, b):
    return lax.dot_general(
        a, b, (((1,), (1,)), ((), ())), precision=HIGHEST, preferred_element_type=f32
    )


def terms_kernel(early, late, q, total, pack):
    top, low = early[0], late[0]
    for k in range(1, BLOCKS + 1):
        top = top + early[k]
        low = low + late[k]
    s = jnp.concatenate([top, low], axis=0)
    total[...] = s
    head = s[:LANES]
    tail = s[LANES:]
    tail_full = jnp.concatenate([tail, jnp.zeros((LANES - TAIL, LANES), f32)], axis=0)
    q_half = q[...].astype(bf16).astype(f32)
    left_tail = dot_t(q_half, tail_full)
    corner = dot_t(tail, tail_full)
    packed_left = left_tail[0:16]
    packed_corner = corner[0:8]
    for j in range(1, 4):
        packed_left = packed_left + pltpu.roll(left_tail[16 * j : 16 * j + 16], 32 * j, 1)
        packed_corner = packed_corner + pltpu.roll(corner[8 * j : 8 * j + 8], 32 * j, 1)
    flat = jnp.concatenate(
        [
            dot_t(q_half, head),
            dot_t(head, head),
            dot_t(tail, head),
            packed_left,
            packed_corner,
            jnp.zeros((8, LANES), f32),
        ],
        axis=0,
    )
    for k in range(SPREAD):
        pack[k] = flat[8 * k : 8 * k + 8]


def terms(early, late, q):
    return pl.pallas_call(
        terms_kernel,
        in_specs=[whole()] * 3,
        out_specs=[whole()] * 2,
        out_shape=[
            jax.ShapeDtypeStruct((ROWS, LANES), f32),
            jax.ShapeDtypeStruct((SPREAD, 8, LANES), f32),
        ],
        name="terms",
        **room(8, 10**8),
    )(early, late, q)


def orthonormal(a, b):
    groups = RANK // 8
    a = [a[8 * i : 8 * i + 8] for i in range(groups)]
    b = [b[8 * i : 8 * i + 8] for i in range(groups)]
    place = lax.broadcasted_iota(jnp.int32, (8, 1), 0)
    for k in range(0, RANK, 2):
        g, r = divmod(k, 8)
        u_a, u_b = a[g][r : r + 1], b[g][r : r + 1]
        w_a, w_b = a[g][r + 1 : r + 2], b[g][r + 1 : r + 2]
        span = range(g, groups)
        by_u = [jnp.sum(a[i] * u_a + b[i] * u_b, axis=1, keepdims=True) for i in span]
        by_w = [jnp.sum(a[i] * w_a + b[i] * w_b, axis=1, keepdims=True) for i in span]
        uu, uw = by_u[0][r : r + 1], by_u[0][r + 1 : r + 2]
        ww = by_w[0][r + 1 : r + 2]
        over_u = 1.0 / (uu + EPS)
        along = uw * over_u
        rest = uw - along * uu
        over_w = 1.0 / (jnp.maximum(ww - along * (uw + rest), 0.0) + EPS)
        w_a = w_a - along * u_a
        w_b = w_b - along * u_b
        for i in span:
            coeff_u = by_u[i - g] * over_u
            coeff_w = (by_w[i - g] - along * by_u[i - g] - coeff_u * rest) * over_w
            if i == g:
                coeff_u = jnp.where(place > r, coeff_u, 0.0)
                coeff_w = jnp.where(place > r + 1, coeff_w, 0.0)
            a[i] = a[i] - coeff_u * u_a - coeff_w * w_a
            b[i] = b[i] - coeff_u * u_b - coeff_w * w_b
    for i in range(groups):
        scale = lax.rsqrt(jnp.sum(a[i] * a[i] + b[i] * b[i], axis=1, keepdims=True) + EPS)
        a[i] = a[i] * scale
        b[i] = b[i] * scale
    return jnp.concatenate(a, axis=0), jnp.concatenate(b, axis=0)


def factor_kernel(pack, s, p_t, p_half, q):
    lane = lax.broadcasted_iota(jnp.int32, (1, LANES), 1)
    keep = lane < TAIL

    def unpack(rows):
        parts = [jnp.where(keep, rows, 0.0)]
        for j in range(1, 4):
            parts.append(jnp.where(keep, pltpu.roll(rows, LANES - 32 * j, 1), 0.0))
        return jnp.concatenate(parts, axis=0)

    flat = jnp.concatenate([pack[k] for k in range(SPREAD)], axis=0)
    empty = jnp.zeros((LANES - TAIL, LANES), f32)
    first_a = flat[0:64]
    gram = flat[64 : 64 + LANES]
    gram_side = jnp.concatenate([flat[64 + LANES : 64 + ROWS], empty], axis=0)
    first_b = unpack(flat[224:240])
    gram_corner = jnp.concatenate([unpack(flat[240:248]), empty], axis=0)

    a, b = orthonormal(first_a, first_b)
    a = a.astype(bf16).astype(f32)
    b = b.astype(bf16).astype(f32)
    second_a = (dot(a, gram) + dot(b, gram_side)) * (1.0 / REPLICAS)
    second_b = (dot_t(a, gram_side) + dot(b, gram_corner)) * (1.0 / REPLICAS)
    a, b = orthonormal(second_a, second_b)
    p_t[:, 0:LANES] = a
    p_t[:, LANES:ROWS] = b[:, 0:TAIL]
    a = a.astype(bf16).astype(f32)
    b = b.astype(bf16).astype(f32)
    p_half[0:LANES, :] = a.T.astype(bf16)
    p_half[LANES:ROWS, :] = b.T[0:TAIL].astype(bf16)
    tail_full = jnp.concatenate([s[LANES:ROWS], empty], axis=0)
    columns = ((dot(a, s[0:LANES]) + dot(b, tail_full)) * (1.0 / REPLICAS)).astype(q.dtype)
    for k in range(8):
        q[k] = columns


def factor(pack, s):
    return pl.pallas_call(
        factor_kernel,
        in_specs=[whole()] * 2,
        out_specs=[whole()] * 3,
        out_shape=[
            jax.ShapeDtypeStruct((RANK, ROWS), f32),
            jax.ShapeDtypeStruct((ROWS, RANK), bf16),
            jax.ShapeDtypeStruct((8, RANK, LANES), bf16),
        ],
        name="factor",
        **room(8, 100000000),
    )(pack, s)


def finish_kernel(n, at, g, e, shrink, p_half, *refs):
    parts, (out, q_t) = refs[:n], refs[-2:]
    shrink = shrink[0:1, 0:1]
    for k in range(n):

        @pl.when(pl.program_id(0) == k)
        def _(part=parts[k]):
            for block in range(BLOCKS):
                cols = slice(block * LANES, (block + 1) * LANES)
                q = part[block]
                approx = jnp.dot(p_half[...], q, preferred_element_type=f32)
                merged = shrink * g[0, :, cols].astype(f32) + e[0, :, cols].astype(f32)
                out[0, :, cols] = merged - approx
                q_t[:, cols] = q.astype(f32)


def finish(at, which, grads, error, shrink, p_half, parts, before=()):
    n = len(parts)

    def column(i, at):
        place = 0
        for k, (other, ahead) in enumerate(which):
            core = 1 - at[0] if other else at[0]
            place = jnp.where(i == k, core * 4 + lax.rem(at[1] + ahead, 4), place)
        return place

    tile = pl.BlockSpec((1, ROWS, QUARTER), lambda i, at: (0, 0, column(i, at)))
    return pl.pallas_call(
        functools.partial(finish_kernel, n),
        grid_spec=pltpu.PrefetchScalarGridSpec(
            num_scalar_prefetch=1,
            grid=(n,),
            in_specs=[
                tile,
                tile,
                pl.BlockSpec((8, LANES), lambda i, at: (0, 0)),
                pl.BlockSpec((ROWS, RANK), lambda i, at: (0, 0)),
            ]
            + [pl.BlockSpec((8, RANK, LANES), lambda i, at: (0, 0, 0))] * n
            + [pl.BlockSpec(memory_space=pl.ANY)] * len(before),
            out_specs=[tile, pl.BlockSpec((RANK, QUARTER), lambda i, at: (0, column(i, at)))],
        ),
        out_shape=[
            jax.ShapeDtypeStruct((1, ROWS, LOCAL), f32),
            jax.ShapeDtypeStruct((RANK, LOCAL), f32),
        ],
        input_output_aliases={5 + n: 0, 6 + n: 1} if before else {},
        name="finish",
        **room(12, 10**9),
    )(at, grads, error, shrink, p_half, *parts, *before)


def respread_kernel(blocks, out):
    total = blocks[0]
    for k in range(1, blocks.shape[0]):
        total = total + blocks[k]
    for k in range(out.shape[0]):
        out[k] = total


def respread(blocks, n):
    return pl.pallas_call(
        respread_kernel,
        in_specs=[whole()],
        out_specs=whole(),
        out_shape=jax.ShapeDtypeStruct((n, *blocks.shape[1:]), f32),
        name="respread",
        **room(4, 1000000),
    )(blocks)


def shifted(value, axis, by):
    n = lax.axis_size(axis)
    return lax.ppermute(value, axis, [(i, (i - by) % n) for i in range(n)])


def swap(value, axis):
    return lax.ppermute(value, axis, [(0, 1), (1, 0)])


def exchange(blocks, axis):
    return lax.all_to_all(blocks, axis, 0, 0, tiled=True)


def from_ring(value, axis):
    return [value] + [shifted(value, axis, j) for j in range(1, 4)]


def to_ring(pieces, axis):
    return [pieces[0]] + [shifted(pieces[j], axis, -j) for j in range(1, 4)]


def step(grads, error, q_init):
    at = jnp.stack([lax.axis_index("c"), lax.axis_index("x"), lax.axis_index("z")]).astype(jnp.int32)
    chip = ("x", "c", "y")
    send, squares, q = prep(at, grads, error, q_init.T)
    got = swap(send, "c")
    squares = exchange(squares, chip)
    *early, squares = merge(early_kernel, at, grads, error, got, squares, 2 * EARLY, (8,))
    early = to_ring(early, "x")
    squares = exchange(squares, "z")
    *late, shrink = merge(late_kernel, at, grads, error, got, squares, LATE, ())
    late = to_ring(late, "x")
    early = fold(fold_early_kernel, EARLY, *early, shrink)
    early = exchange(early, "z")
    late = exchange(fold(fold_late_kernel, LATE, *late, early), "z")
    s, pack = terms(early, late, q)

    pack = respread(exchange(pack, chip), 8)
    pack = exchange(respread(exchange(pack, "z"), SPREAD), chip)

    p_t, p_half, q = factor(pack, s)
    parts = from_ring(exchange(q, "z"), "x")
    others = [swap(part, "c") for part in parts]
    args = (grads, error, shrink, p_half)
    outs = finish(at, [(0, 0), (1, 0)], *args, [parts[0], others[0]])
    outs = finish(at, [(0, 1), (0, 2), (0, 3)], *args, parts[1:], outs)
    new_error, q_t = finish(at, [(1, 1), (1, 2), (1, 3)], *args, others[1:], outs)
    return p_t.T, q_t.T, new_error


def solution(mesh):
    finer = Mesh(
        mesh.devices.reshape(8, 4, 2, mesh.shape["tensor"]), ("z", "x", "c", "y")
    )
    replicas = ("z", "x", "c")
    return jax.shard_map(
        step,
        mesh=finer,
        in_specs=(P(replicas, None, "y"), P(replicas, None, "y"), P("y", None)),
        out_specs=(P(), P("y", None), P(replicas, None, "y")),
        check_vma=False,
    )
```

```python
import functools

import jax
import jax.numpy as jnp
from jax import lax
from jax.experimental import pallas as pl
from jax.experimental.pallas import tpu as pltpu
from jax.sharding import Mesh
from jax.sharding import PartitionSpec as P


ROWS = 160
COLS = 28672
RANK = 64
LOCAL = 7168
HALF = LOCAL // 2
QUARTER = HALF // 4
LANES = 128
BLOCKS = QUARTER // LANES
TAIL = ROWS - LANES
EARLY = 48
LATE = ROWS - EARLY
SPREAD = 32
REPLICAS = 64
EPS = 1e-06
CLIP = 0.5

f32 = jnp.float32
bf16 = jnp.bfloat16
HIGHEST = lax.Precision.HIGHEST
VMEM = pltpu.VMEM


def whole():
    return pl.BlockSpec(memory_space=VMEM)


def room(mib, flops=10**6):
    return dict(
        compiler_params=pltpu.CompilerParams(vmem_limit_bytes=mib * 2**20),
        cost_estimate=pl.CostEstimate(flops=flops, bytes_accessed=2**20, transcendentals=0),
    )


def shrink_of(squares):
    rows = jnp.sum(squares, axis=0)
    total = jnp.sum(jnp.sum(rows, axis=1, keepdims=True), axis=0, keepdims=True)
    scaled = CLIP * jnp.sqrt(f32(ROWS * COLS))
    return jnp.minimum(1.0, scaled * lax.rsqrt(total / REPLICAS + EPS))


def prep_kernel(g, e, q_all, send, squares, q, at, other, own, sems):
    core, x, z = (lax.axis_index(axis) for axis in ("c", "x", "z"))
    at[0], at[1], at[2] = core, x, z

    def piece(ref, core, out, sem):
        cols = pl.ds(pl.multiple_of(core * HALF, LANES), HALF)
        return pltpu.make_async_copy(ref.at[0, :, cols], out, sems.at[sem])

    top, low = slice(0, ROWS), slice(ROWS, 2 * ROWS)
    first = core * 4 * BLOCKS + x * BLOCKS + jnp.minimum(z, BLOCKS - 1)
    cols = pl.ds(pl.multiple_of(first * LANES, LANES), LANES)
    copies = [
        piece(g, 1 - core, other.at[top], 0),
        piece(g, core, own, 1),
        piece(e, 1 - core, other.at[low], 2),
        pltpu.make_async_copy(q_all.at[:, cols], q, sems.at[3]),
    ]
    out = [
        pltpu.make_async_copy(other.at[part], send.at[part], sems.at[4 + k])
        for k, part in enumerate((top, low))
    ]
    for copy in copies:
        copy.start()

    def rows_of(ref):
        def rows(i, acc):
            for lane in range(0, HALF, HALF // 4):
                block = ref[pl.ds(i * 16, 16), lane : lane + HALF // 4].astype(f32)
                block = block * block
                acc = acc + (block[:8] + block[8:])
            return acc

        return rows

    acc = jnp.zeros((8, HALF // 4), f32)
    copies[0].wait()
    out[0].start()
    acc = lax.fori_loop(0, ROWS // 16, rows_of(other), acc)
    copies[1].wait()
    copies[2].wait()
    out[1].start()
    acc = lax.fori_loop(0, ROWS // 16, rows_of(own), acc)
    part = acc[:, :LANES]
    for lane in range(LANES, HALF // 4, LANES):
        part = part + acc[:, lane : lane + LANES]
    for k in range(SPREAD):
        squares[k] = part
    copies[3].wait()
    for copy in out:
        copy.wait()


def prep(grads, error, q_t):
    hbm = pl.BlockSpec(memory_space=pltpu.HBM)
    return pl.pallas_call(
        prep_kernel,
        in_specs=[hbm, hbm, hbm],
        out_specs=[hbm, whole(), whole(), pl.BlockSpec(memory_space=pltpu.SMEM)],
        scratch_shapes=[
            VMEM((2 * ROWS, HALF), bf16),
            VMEM((ROWS, HALF), bf16),
            pltpu.SemaphoreType.DMA((6,)),
        ],
        out_shape=[
            jax.ShapeDtypeStruct((2 * ROWS, HALF), bf16),
            jax.ShapeDtypeStruct((SPREAD, 8, LANES), f32),
            jax.ShapeDtypeStruct((RANK, LANES), f32),
            jax.ShapeDtypeStruct((3,), jnp.int32),
        ],
        name="prep",
        **room(58, 10**8),
    )(grads, error, q_t)


def both(g, e, got, row, cols):
    here = pl.ds(row, 16)
    gradient = g[0, here, cols].astype(f32) + got[here, cols].astype(f32)
    residue = e[0, here, cols].astype(f32) + got[pl.ds(ROWS + row, 16), cols].astype(f32)
    return gradient, residue


def early_kernel(at, g, e, got, squares, *outs):
    outs, spread = outs[:4], outs[4]
    for j, out in enumerate(outs):
        cols = pl.ds(pl.multiple_of(lax.rem(at[1] + j, 4) * QUARTER, LANES), QUARTER)

        def rows(i, carry, out=out, cols=cols):
            gradient, residue = both(g, e, got, i * 16, cols)
            out[pl.ds(i * 16, 16), :] = gradient
            out[pl.ds(EARLY + i * 16, 16), :] = residue
            return carry

        lax.fori_loop(0, EARLY // 16, rows, 0)
    total = jnp.sum(squares[...], axis=0)
    for k in range(8):
        spread[k] = total


def late_kernel(at, g, e, got, squares, *outs):
    outs, spread = outs[:4], outs[4]
    shrink = shrink_of(squares[...])
    spread[...] = jnp.broadcast_to(shrink, (8, LANES))
    for j, out in enumerate(outs):
        cols = pl.ds(pl.multiple_of(lax.rem(at[1] + j, 4) * QUARTER, LANES), QUARTER)

        def rows(i, carry, out=out, cols=cols):
            gradient, residue = both(g, e, got, EARLY + i * 16, cols)
            out[pl.ds(i * 16, 16), :] = shrink * gradient + residue
            return carry

        lax.fori_loop(0, LATE // 16, rows, 0)


def merge(kernel, at, grads, error, got, squares, rows, spread):
    own = pl.BlockSpec((1, ROWS, HALF), lambda i, at: (0, 0, at[0]))
    outs = [((rows, QUARTER), f32)] * 4
    outs = outs + [((*spread, 8, LANES), f32)]
    return pl.pallas_call(
        kernel,
        grid_spec=pltpu.PrefetchScalarGridSpec(
            num_scalar_prefetch=1,
            grid=(1,),
            in_specs=[
                own,
                own,
                pl.BlockSpec((2 * ROWS, HALF), lambda i, at: (0, 0)),
                pl.BlockSpec(squares.shape, lambda i, at: (0, 0, 0)),
            ],
            out_specs=[
                pl.BlockSpec(shape, lambda i, at, shape=shape: (0,) * len(shape))
                for shape, _ in outs
            ],
        ),
        out_shape=[jax.ShapeDtypeStruct(*out) for out in outs],
        **room(16, 10**9),
    )(at, grads, error, got, squares)


def fold_early_kernel(a, b, c, d, shrink, out):
    shrink = shrink[0:1, 0:1]
    top, low = slice(0, EARLY), slice(EARLY, 2 * EARLY)
    for k in range(BLOCKS):
        cols = slice(k * LANES, (k + 1) * LANES)
        gradient = (a[top, cols] + c[top, cols]) + (b[top, cols] + d[top, cols])
        residue = (a[low, cols] + c[low, cols]) + (b[low, cols] + d[low, cols])
        out[k] = shrink * gradient + residue
    out[BLOCKS] = jnp.zeros((EARLY, LANES), f32)


def fold_late_kernel(a, b, c, d, after, out):
    for k in range(BLOCKS):
        cols = slice(k * LANES, (k + 1) * LANES)
        out[k] = (a[:, cols] + c[:, cols]) + (b[:, cols] + d[:, cols])
    out[BLOCKS] = jnp.zeros((LATE, LANES), f32)


def fold(kernel, rows, *args):
    return pl.pallas_call(
        kernel,
        in_specs=[whole()] * len(args),
        out_specs=whole(),
        out_shape=jax.ShapeDtypeStruct((BLOCKS + 1, rows, LANES), f32),
        **room(8, 10**8),
    )(*args)


def dot(a, b):
    return jnp.dot(a, b, precision=HIGHEST, preferred_element_type=f32)


def dot_t(a, b):
    return lax.dot_general(
        a, b, (((1,), (1,)), ((), ())), precision=HIGHEST, preferred_element_type=f32
    )


def terms_kernel(early, late, q, total, pack):
    top, low = early[0], late[0]
    for k in range(1, BLOCKS + 1):
        top = top + early[k]
        low = low + late[k]
    s = jnp.concatenate([top, low], axis=0)
    total[...] = s
    head = s[:LANES]
    tail = s[LANES:]
    tail_full = jnp.concatenate([tail, jnp.zeros((LANES - TAIL, LANES), f32)], axis=0)
    q_half = q[...].astype(bf16).astype(f32)
    left_tail = dot_t(q_half, tail_full)
    corner = dot_t(tail, tail_full)
    packed_left = left_tail[0:16]
    packed_corner = corner[0:8]
    for j in range(1, 4):
        packed_left = packed_left + pltpu.roll(left_tail[16 * j : 16 * j + 16], 32 * j, 1)
        packed_corner = packed_corner + pltpu.roll(corner[8 * j : 8 * j + 8], 32 * j, 1)
    flat = jnp.concatenate(
        [
            dot_t(q_half, head),
            dot_t(head, head),
            dot_t(tail, head),
            packed_left,
            packed_corner,
            jnp.zeros((8, LANES), f32),
        ],
        axis=0,
    )
    for k in range(SPREAD):
        pack[k] = flat[8 * k : 8 * k + 8]


def terms(early, late, q):
    return pl.pallas_call(
        terms_kernel,
        in_specs=[whole()] * 3,
        out_specs=[whole()] * 2,
        out_shape=[
            jax.ShapeDtypeStruct((ROWS, LANES), f32),
            jax.ShapeDtypeStruct((SPREAD, 8, LANES), f32),
        ],
        name="terms",
        **room(8, 10**8),
    )(early, late, q)


def across(value):
    return jnp.broadcast_to(jnp.sum(value, axis=1, keepdims=True), value.shape)


def orthonormal(a, b):
    groups = RANK // 8
    a = [a[8 * i : 8 * i + 8] for i in range(groups)]
    b = [b[8 * i : 8 * i + 8] for i in range(groups)]
    place = lax.broadcasted_iota(jnp.int32, (8, LANES), 0)
    for k in range(0, RANK, 2):
        g, r = divmod(k, 8)
        u_a, u_b = a[g][r : r + 1], b[g][r : r + 1]
        w_a, w_b = a[g][r + 1 : r + 2], b[g][r + 1 : r + 2]
        span = range(g, groups)
        by_u = [across(a[i] * u_a + b[i] * u_b) for i in span]
        by_w = [across(a[i] * w_a + b[i] * w_b) for i in span]
        uu, uw = by_u[0][r : r + 1], by_u[0][r + 1 : r + 2]
        ww = by_w[0][r + 1 : r + 2]
        over_u = 1.0 / (uu + EPS)
        along = uw * over_u
        rest = uw - along * uu
        over_w = 1.0 / (jnp.maximum(ww - along * (uw + rest), 0.0) + EPS)
        w_a = w_a - along * u_a
        w_b = w_b - along * u_b
        for i in span:
            coeff_u = by_u[i - g] * over_u
            coeff_w = (by_w[i - g] - along * by_u[i - g] - coeff_u * rest) * over_w
            if i == g:
                coeff_u = jnp.where(place > r, coeff_u, 0.0)
                coeff_w = jnp.where(place > r + 1, coeff_w, 0.0)
            a[i] = a[i] - coeff_u * u_a - coeff_w * w_a
            b[i] = b[i] - coeff_u * u_b - coeff_w * w_b
    for i in range(groups):
        scale = lax.rsqrt(across(a[i] * a[i] + b[i] * b[i]) + EPS)
        a[i] = a[i] * scale
        b[i] = b[i] * scale
    return jnp.concatenate(a, axis=0), jnp.concatenate(b, axis=0)


def factor_kernel(pack, s, p_t, p_half, q):
    lane = lax.broadcasted_iota(jnp.int32, (1, LANES), 1)
    keep = lane < TAIL

    def unpack(rows):
        parts = [jnp.where(keep, rows, 0.0)]
        for j in range(1, 4):
            parts.append(jnp.where(keep, pltpu.roll(rows, LANES - 32 * j, 1), 0.0))
        return jnp.concatenate(parts, axis=0)

    flat = jnp.concatenate([pack[k] for k in range(SPREAD)], axis=0)
    empty = jnp.zeros((LANES - TAIL, LANES), f32)
    first_a = flat[0:64]
    gram = flat[64 : 64 + LANES]
    gram_side = jnp.concatenate([flat[64 + LANES : 64 + ROWS], empty], axis=0)
    first_b = unpack(flat[224:240])
    gram_corner = jnp.concatenate([unpack(flat[240:248]), empty], axis=0)

    a, b = orthonormal(first_a, first_b)
    a = a.astype(bf16).astype(f32)
    b = b.astype(bf16).astype(f32)
    second_a = (dot(a, gram) + dot(b, gram_side)) * (1.0 / REPLICAS)
    second_b = (dot_t(a, gram_side) + dot(b, gram_corner)) * (1.0 / REPLICAS)
    a, b = orthonormal(second_a, second_b)
    p_t[:, 0:LANES] = a
    p_t[:, LANES:ROWS] = b[:, 0:TAIL]
    a = a.astype(bf16).astype(f32)
    b = b.astype(bf16).astype(f32)
    p_half[0:LANES, :] = a.T.astype(bf16)
    p_half[LANES:ROWS, :] = b.T[0:TAIL].astype(bf16)
    tail_full = jnp.concatenate([s[LANES:ROWS], empty], axis=0)
    columns = ((dot(a, s[0:LANES]) + dot(b, tail_full)) * (1.0 / REPLICAS)).astype(q.dtype)
    for k in range(8):
        q[k] = columns


def factor(pack, s):
    return pl.pallas_call(
        factor_kernel,
        in_specs=[whole()] * 2,
        out_specs=[whole()] * 3,
        out_shape=[
            jax.ShapeDtypeStruct((RANK, ROWS), f32),
            jax.ShapeDtypeStruct((ROWS, RANK), bf16),
            jax.ShapeDtypeStruct((8, RANK, LANES), bf16),
        ],
        name="factor",
        **room(8, 100000000),
    )(pack, s)


def place_of(which, i, at):
    place = 0
    for k, (other, ahead) in enumerate(which):
        core = 1 - at[0] if other else at[0]
        place = jnp.where(i == k, core * 4 + lax.rem(at[1] + ahead, 4), place)
    return place


def finish_kernel(which, at, g, e, shrink, p_half, *refs):
    n = len(which)
    parts, (out, q_t) = refs[:n], refs[-2:]
    shrink = shrink[0:1, 0:1]
    step = pl.program_id(0)
    first = place_of(which, step, at) * QUARTER
    for k in range(n):

        @pl.when(step == k)
        def _(part=parts[k]):
            for block in range(BLOCKS):
                cols = slice(block * LANES, (block + 1) * LANES)
                here = pl.ds(pl.multiple_of(first + block * LANES, LANES), LANES)
                q = part[block]
                approx = jnp.dot(p_half[...], q, preferred_element_type=f32)
                merged = shrink * g[0, :, here].astype(f32) + e[0, :, here].astype(f32)
                out[0, :, cols] = merged - approx
                q_t[:, cols] = q.astype(f32)


def finish(at, which, grads, error, shrink, p_half, parts, before=()):
    n = len(parts)
    column = functools.partial(place_of, which)
    return pl.pallas_call(
        functools.partial(finish_kernel, which),
        grid_spec=pltpu.PrefetchScalarGridSpec(
            num_scalar_prefetch=1,
            grid=(n,),
            in_specs=[whole()] * (4 + n) + [pl.BlockSpec(memory_space=pl.ANY)] * len(before),
            out_specs=[
                pl.BlockSpec((1, ROWS, QUARTER), lambda i, at: (0, 0, column(i, at))),
                pl.BlockSpec((RANK, QUARTER), lambda i, at: (0, column(i, at))),
            ],
        ),
        out_shape=[
            jax.ShapeDtypeStruct((1, ROWS, LOCAL), f32),
            jax.ShapeDtypeStruct((RANK, LOCAL), f32),
        ],
        input_output_aliases={5 + n: 0, 6 + n: 1} if before else {},
        name="finish",
        **room(12, 10**9),
    )(at, grads, error, shrink, p_half, *parts, *before)


def respread_kernel(blocks, out):
    total = blocks[0]
    for k in range(1, blocks.shape[0]):
        total = total + blocks[k]
    for k in range(out.shape[0]):
        out[k] = total


def respread(blocks, n):
    return pl.pallas_call(
        respread_kernel,
        in_specs=[whole()],
        out_specs=whole(),
        out_shape=jax.ShapeDtypeStruct((n, *blocks.shape[1:]), f32),
        name="respread",
        **room(4, 1000000),
    )(blocks)


def shifted(value, axis, by):
    n = lax.axis_size(axis)
    return lax.ppermute(value, axis, [(i, (i - by) % n) for i in range(n)])


def swap(value, axis):
    return lax.ppermute(value, axis, [(0, 1), (1, 0)])


def exchange(blocks, axis):
    return lax.all_to_all(blocks, axis, 0, 0, tiled=True)


def from_ring(value, axis):
    return [value] + [shifted(value, axis, j) for j in range(1, 4)]


def to_ring(pieces, axis):
    return [pieces[0]] + [shifted(pieces[j], axis, -j) for j in range(1, 4)]


def step(grads, error, q_init):
    chip = ("x", "c", "y")
    send, squares, q, at = prep(grads, error, q_init.T)
    got = swap(send, "c")
    squares = exchange(squares, chip)
    *early, squares = merge(early_kernel, at, grads, error, got, squares, 2 * EARLY, (8,))
    early = to_ring(early, "x")
    squares = exchange(squares, "z")
    *late, shrink = merge(late_kernel, at, grads, error, got, squares, LATE, ())
    late = to_ring(late, "x")
    early = fold(fold_early_kernel, EARLY, *early, shrink)
    early = exchange(early, "z")
    late = exchange(fold(fold_late_kernel, LATE, *late, early), "z")
    s, pack = terms(early, late, q)

    pack = respread(exchange(pack, chip), 8)
    pack = exchange(respread(exchange(pack, "z"), SPREAD), chip)

    p_t, p_half, q = factor(pack, s)
    q = exchange(q, "z")
    parts = from_ring(q, "x")
    others = [swap(part, "c") for part in parts]
    args = (grads, error, shrink, p_half)
    outs = finish(at, [(0, 0), (1, 0)], *args, [parts[0], others[0]])
    outs = finish(at, [(0, 1), (0, 2), (0, 3)], *args, parts[1:], outs)
    new_error, q_t = finish(at, [(1, 1), (1, 2), (1, 3)], *args, others[1:], outs)
    return p_t.T, q_t.T, new_error


def solution(mesh):
    finer = Mesh(
        mesh.devices.reshape(8, 4, 2, mesh.shape["tensor"]), ("z", "x", "c", "y")
    )
    replicas = ("z", "x", "c")
    return jax.shard_map(
        step,
        mesh=finer,
        in_specs=(P(replicas, None, "y"), P(replicas, None, "y"), P("y", None)),
        out_specs=(P(), P("y", None), P(replicas, None, "y")),
        check_vma=False,
    )
```

```python
import functools

import jax
import jax.numpy as jnp
from jax import lax
from jax.experimental import pallas as pl
from jax.experimental.pallas import tpu as pltpu
from jax.sharding import Mesh
from jax.sharding import PartitionSpec as P


ROWS = 160
COLS = 28672
RANK = 64
LOCAL = 7168
HALF = LOCAL // 2
QUARTER = HALF // 4
LANES = 128
BLOCKS = QUARTER // LANES
TAIL = ROWS - LANES
EARLY = 48
LATE = ROWS - EARLY
SPREAD = 32
REPLICAS = 64
EPS = 1e-06
CLIP = 0.5

f32 = jnp.float32
bf16 = jnp.bfloat16
HIGHEST = lax.Precision.HIGHEST
VMEM = pltpu.VMEM


def whole():
    return pl.BlockSpec(memory_space=VMEM)


def room(mib, flops=10**6):
    return dict(
        compiler_params=pltpu.CompilerParams(vmem_limit_bytes=mib * 2**20),
        cost_estimate=pl.CostEstimate(flops=flops, bytes_accessed=2**20, transcendentals=0),
    )


def shrink_of(squares):
    rows = jnp.sum(squares, axis=0)
    total = jnp.sum(jnp.sum(rows, axis=1, keepdims=True), axis=0, keepdims=True)
    scaled = CLIP * jnp.sqrt(f32(ROWS * COLS))
    return jnp.minimum(1.0, scaled * lax.rsqrt(total / REPLICAS + EPS))


def prep_kernel(g, e, q_all, send, squares, q, other, own, sems):
    core, x, z = (lax.axis_index(axis) for axis in ("c", "x", "z"))

    def piece(ref, core, out, sem):
        cols = pl.ds(pl.multiple_of(core * HALF, LANES), HALF)
        return pltpu.make_async_copy(ref.at[0, :, cols], out, sems.at[sem])

    top, low = slice(0, ROWS), slice(ROWS, 2 * ROWS)
    first = core * 4 * BLOCKS + x * BLOCKS + jnp.minimum(z, BLOCKS - 1)
    cols = pl.ds(pl.multiple_of(first * LANES, LANES), LANES)
    copies = [
        piece(g, 1 - core, other.at[top], 0),
        piece(g, core, own, 1),
        piece(e, 1 - core, other.at[low], 2),
        pltpu.make_async_copy(q_all.at[:, cols], q, sems.at[3]),
    ]
    out = [
        pltpu.make_async_copy(other.at[part], send.at[part], sems.at[4 + k])
        for k, part in enumerate((top, low))
    ]
    for copy in copies:
        copy.start()

    def rows_of(ref):
        def rows(i, acc):
            for lane in range(0, HALF, HALF // 4):
                block = ref[pl.ds(i * 16, 16), lane : lane + HALF // 4].astype(f32)
                block = block * block
                acc = acc + (block[:8] + block[8:])
            return acc

        return rows

    acc = jnp.zeros((8, HALF // 4), f32)
    copies[0].wait()
    out[0].start()
    acc = lax.fori_loop(0, ROWS // 16, rows_of(other), acc)
    copies[1].wait()
    copies[2].wait()
    out[1].start()
    acc = lax.fori_loop(0, ROWS // 16, rows_of(own), acc)
    part = acc[:, :LANES]
    for lane in range(LANES, HALF // 4, LANES):
        part = part + acc[:, lane : lane + LANES]
    for k in range(SPREAD):
        squares[k] = part
    copies[3].wait()
    for copy in out:
        copy.wait()


def prep(grads, error, q_t):
    hbm = pl.BlockSpec(memory_space=pltpu.HBM)
    return pl.pallas_call(
        prep_kernel,
        in_specs=[hbm, hbm, hbm],
        out_specs=[hbm, whole(), whole()],
        scratch_shapes=[
            VMEM((2 * ROWS, HALF), bf16),
            VMEM((ROWS, HALF), bf16),
            pltpu.SemaphoreType.DMA((6,)),
        ],
        out_shape=[
            jax.ShapeDtypeStruct((2 * ROWS, HALF), bf16),
            jax.ShapeDtypeStruct((SPREAD, 8, LANES), f32),
            jax.ShapeDtypeStruct((RANK, LANES), f32),
        ],
        name="prep",
        **room(58, 10**8),
    )(grads, error, q_t)


def both(g, e, got, row, core, place):
    here = pl.ds(row, 16)
    mine = pl.ds(pl.multiple_of(core * HALF + place * QUARTER, LANES), QUARTER)
    cols = pl.ds(pl.multiple_of(place * QUARTER, LANES), QUARTER)
    gradient = g[0, here, mine].astype(f32) + got[here, cols].astype(f32)
    residue = e[0, here, mine].astype(f32) + got[pl.ds(ROWS + row, 16), cols].astype(f32)
    return gradient, residue


def early_kernel(g, e, got, squares, *outs):
    outs, spread = outs[:4], outs[4]
    core, x = lax.axis_index("c"), lax.axis_index("x")
    for j, out in enumerate(outs):
        place = lax.rem(x + j, 4)

        def rows(i, carry, out=out, place=place):
            gradient, residue = both(g, e, got, i * 16, core, place)
            out[pl.ds(i * 16, 16), :] = gradient
            out[pl.ds(EARLY + i * 16, 16), :] = residue
            return carry

        lax.fori_loop(0, EARLY // 16, rows, 0)
    total = jnp.sum(squares[...], axis=0)
    for k in range(8):
        spread[k] = total


def late_kernel(g, e, got, squares, *outs):
    outs, spread = outs[:4], outs[4]
    core, x = lax.axis_index("c"), lax.axis_index("x")
    shrink = shrink_of(squares[...])
    spread[...] = jnp.broadcast_to(shrink, (8, LANES))
    for j, out in enumerate(outs):
        place = lax.rem(x + j, 4)

        def rows(i, carry, out=out, place=place):
            gradient, residue = both(g, e, got, EARLY + i * 16, core, place)
            out[pl.ds(i * 16, 16), :] = shrink * gradient + residue
            return carry

        lax.fori_loop(0, LATE // 16, rows, 0)


def merge(kernel, grads, error, got, squares, rows, spread):
    outs = [(rows, QUARTER)] * 4 + [(*spread, 8, LANES)]
    return pl.pallas_call(
        kernel,
        in_specs=[whole()] * 4,
        out_specs=[whole()] * len(outs),
        out_shape=[jax.ShapeDtypeStruct(shape, f32) for shape in outs],
        **room(16, 10**9),
    )(grads, error, got, squares)


def fold_early_kernel(a, b, c, d, shrink, out):
    shrink = shrink[0:1, 0:1]
    top, low = slice(0, EARLY), slice(EARLY, 2 * EARLY)
    for k in range(BLOCKS):
        cols = slice(k * LANES, (k + 1) * LANES)
        gradient = (a[top, cols] + c[top, cols]) + (b[top, cols] + d[top, cols])
        residue = (a[low, cols] + c[low, cols]) + (b[low, cols] + d[low, cols])
        out[k] = shrink * gradient + residue
    out[BLOCKS] = jnp.zeros((EARLY, LANES), f32)


def fold_late_kernel(a, b, c, d, after, out):
    for k in range(BLOCKS):
        cols = slice(k * LANES, (k + 1) * LANES)
        out[k] = (a[:, cols] + c[:, cols]) + (b[:, cols] + d[:, cols])
    out[BLOCKS] = jnp.zeros((LATE, LANES), f32)


def fold(kernel, rows, *args):
    return pl.pallas_call(
        kernel,
        in_specs=[whole()] * len(args),
        out_specs=whole(),
        out_shape=jax.ShapeDtypeStruct((BLOCKS + 1, rows, LANES), f32),
        **room(8, 10**8),
    )(*args)


def dot(a, b):
    return jnp.dot(a, b, precision=HIGHEST, preferred_element_type=f32)


def dot_t(a, b):
    return lax.dot_general(
        a, b, (((1,), (1,)), ((), ())), precision=HIGHEST, preferred_element_type=f32
    )


def terms_kernel(early, late, q, total, pack):
    top, low = early[0], late[0]
    for k in range(1, BLOCKS + 1):
        top = top + early[k]
        low = low + late[k]
    s = jnp.concatenate([top, low], axis=0)
    total[...] = s
    head = s[:LANES]
    tail = s[LANES:]
    tail_full = jnp.concatenate([tail, jnp.zeros((LANES - TAIL, LANES), f32)], axis=0)
    q_half = q[...].astype(bf16).astype(f32)
    left_tail = dot_t(q_half, tail_full)
    corner = dot_t(tail, tail_full)
    packed_left = left_tail[0:16]
    packed_corner = corner[0:8]
    for j in range(1, 4):
        packed_left = packed_left + pltpu.roll(left_tail[16 * j : 16 * j + 16], 32 * j, 1)
        packed_corner = packed_corner + pltpu.roll(corner[8 * j : 8 * j + 8], 32 * j, 1)
    flat = jnp.concatenate(
        [
            dot_t(q_half, head),
            dot_t(head, head),
            dot_t(tail, head),
            packed_left,
            packed_corner,
            jnp.zeros((8, LANES), f32),
        ],
        axis=0,
    )
    for k in range(SPREAD):
        pack[k] = flat[8 * k : 8 * k + 8]


def terms(early, late, q):
    return pl.pallas_call(
        terms_kernel,
        in_specs=[whole()] * 3,
        out_specs=[whole()] * 2,
        out_shape=[
            jax.ShapeDtypeStruct((ROWS, LANES), f32),
            jax.ShapeDtypeStruct((SPREAD, 8, LANES), f32),
        ],
        name="terms",
        **room(8, 10**8),
    )(early, late, q)


def across(value):
    return jnp.broadcast_to(jnp.sum(value, axis=1, keepdims=True), value.shape)


def orthonormal(a, b):
    groups = RANK // 8
    a = [a[8 * i : 8 * i + 8] for i in range(groups)]
    b = [b[8 * i : 8 * i + 8] for i in range(groups)]
    place = lax.broadcasted_iota(jnp.int32, (8, LANES), 0)
    for k in range(0, RANK, 2):
        g, r = divmod(k, 8)
        u_a, u_b = a[g][r : r + 1], b[g][r : r + 1]
        w_a, w_b = a[g][r + 1 : r + 2], b[g][r + 1 : r + 2]
        span = range(g, groups)
        by_u = [across(a[i] * u_a + b[i] * u_b) for i in span]
        by_w = [across(a[i] * w_a + b[i] * w_b) for i in span]
        uu, uw = by_u[0][r : r + 1], by_u[0][r + 1 : r + 2]
        ww = by_w[0][r + 1 : r + 2]
        over_u = 1.0 / (uu + EPS)
        along = uw * over_u
        rest = uw - along * uu
        over_w = 1.0 / (jnp.maximum(ww - along * (uw + rest), 0.0) + EPS)
        w_a = w_a - along * u_a
        w_b = w_b - along * u_b
        for i in span:
            coeff_u = by_u[i - g] * over_u
            coeff_w = (by_w[i - g] - along * by_u[i - g] - coeff_u * rest) * over_w
            if i == g:
                coeff_u = jnp.where(place > r, coeff_u, 0.0)
                coeff_w = jnp.where(place > r + 1, coeff_w, 0.0)
            a[i] = a[i] - coeff_u * u_a - coeff_w * w_a
            b[i] = b[i] - coeff_u * u_b - coeff_w * w_b
    for i in range(groups):
        scale = lax.rsqrt(across(a[i] * a[i] + b[i] * b[i]) + EPS)
        a[i] = a[i] * scale
        b[i] = b[i] * scale
    return jnp.concatenate(a, axis=0), jnp.concatenate(b, axis=0)


def factor_kernel(pack, s, p_t, p_half, q):
    lane = lax.broadcasted_iota(jnp.int32, (1, LANES), 1)
    keep = lane < TAIL

    def unpack(rows):
        parts = [jnp.where(keep, rows, 0.0)]
        for j in range(1, 4):
            parts.append(jnp.where(keep, pltpu.roll(rows, LANES - 32 * j, 1), 0.0))
        return jnp.concatenate(parts, axis=0)

    flat = jnp.concatenate([pack[k] for k in range(SPREAD)], axis=0)
    empty = jnp.zeros((LANES - TAIL, LANES), f32)
    first_a = flat[0:64]
    gram = flat[64 : 64 + LANES]
    gram_side = jnp.concatenate([flat[64 + LANES : 64 + ROWS], empty], axis=0)
    first_b = unpack(flat[224:240])
    gram_corner = jnp.concatenate([unpack(flat[240:248]), empty], axis=0)

    a, b = orthonormal(first_a, first_b)
    a = a.astype(bf16).astype(f32)
    b = b.astype(bf16).astype(f32)
    second_a = (dot(a, gram) + dot(b, gram_side)) * (1.0 / REPLICAS)
    second_b = (dot_t(a, gram_side) + dot(b, gram_corner)) * (1.0 / REPLICAS)
    a, b = orthonormal(second_a, second_b)
    p_t[:, 0:LANES] = a
    p_t[:, LANES:ROWS] = b[:, 0:TAIL]
    a = a.astype(bf16).astype(f32)
    b = b.astype(bf16).astype(f32)
    p_half[0:LANES, :] = a.T.astype(bf16)
    p_half[LANES:ROWS, :] = b.T[0:TAIL].astype(bf16)
    tail_full = jnp.concatenate([s[LANES:ROWS], empty], axis=0)
    columns = ((dot(a, s[0:LANES]) + dot(b, tail_full)) * (1.0 / REPLICAS)).astype(q.dtype)
    for k in range(8):
        q[k] = columns


def factor(pack, s):
    return pl.pallas_call(
        factor_kernel,
        in_specs=[whole()] * 2,
        out_specs=[whole()] * 3,
        out_shape=[
            jax.ShapeDtypeStruct((RANK, ROWS), f32),
            jax.ShapeDtypeStruct((ROWS, RANK), bf16),
            jax.ShapeDtypeStruct((8, RANK, LANES), bf16),
        ],
        name="factor",
        **room(8, 100000000),
    )(pack, s)


def finish_kernel(which, g, e, shrink, p_half, *refs):
    n = len(which)
    parts = refs[:n]
    out, q_t, new, right_part, sems = refs[-5:]
    shrink = shrink[0:1, 0:1]
    core, x = lax.axis_index("c"), lax.axis_index("x")
    copies = []
    for k, (other, ahead) in enumerate(which):
        place = (1 - core if other else core) * 4 + lax.rem(x + ahead, 4)
        first = place * QUARTER
        for block in range(BLOCKS):
            cols = slice(block * LANES, (block + 1) * LANES)
            here = pl.ds(pl.multiple_of(first + block * LANES, LANES), LANES)
            q = parts[k][block]
            approx = jnp.dot(p_half[...], q, preferred_element_type=f32)
            merged = shrink * g[0, :, here].astype(f32) + e[0, :, here].astype(f32)
            new[k, :, cols] = merged - approx
            right_part[k, :, cols] = q.astype(f32)
        cols = pl.ds(pl.multiple_of(first, LANES), QUARTER)
        for j, rows in enumerate((slice(0, ROWS // 2), slice(ROWS // 2, ROWS))):
            copies.append(
                pltpu.make_async_copy(new.at[k, rows], out.at[0, rows, cols], sems.at[3 * k + j])
            )
        copies.append(pltpu.make_async_copy(right_part.at[k], q_t.at[:, cols], sems.at[3 * k + 2]))
        for copy in copies[-3:]:
            copy.start()
    for copy in copies:
        copy.wait()


def finish(which, grads, error, shrink, p_half, parts, before=()):
    n = len(parts)
    hbm = pl.BlockSpec(memory_space=pltpu.HBM)
    return pl.pallas_call(
        functools.partial(finish_kernel, which),
        in_specs=[whole()] * (4 + n) + [hbm] * len(before),
        out_specs=[hbm, hbm],
        scratch_shapes=[
            VMEM((n, ROWS, QUARTER), f32),
            VMEM((n, RANK, QUARTER), f32),
            pltpu.SemaphoreType.DMA((3 * n,)),
        ],
        out_shape=[
            jax.ShapeDtypeStruct((1, ROWS, LOCAL), f32),
            jax.ShapeDtypeStruct((RANK, LOCAL), f32),
        ],
        input_output_aliases={4 + n: 0, 5 + n: 1} if before else {},
        name="finish",
        **room(12, 10**9),
    )(grads, error, shrink, p_half, *parts, *before)


def respread_kernel(blocks, out):
    total = blocks[0]
    for k in range(1, blocks.shape[0]):
        total = total + blocks[k]
    for k in range(out.shape[0]):
        out[k] = total


def respread(blocks, n):
    return pl.pallas_call(
        respread_kernel,
        in_specs=[whole()],
        out_specs=whole(),
        out_shape=jax.ShapeDtypeStruct((n, *blocks.shape[1:]), f32),
        name="respread",
        **room(4, 1000000),
    )(blocks)


def shifted(value, axis, by):
    n = lax.axis_size(axis)
    return lax.ppermute(value, axis, [(i, (i - by) % n) for i in range(n)])


def swap(value, axis):
    return lax.ppermute(value, axis, [(0, 1), (1, 0)])


def exchange(blocks, axis):
    return lax.all_to_all(blocks, axis, 0, 0, tiled=True)


def from_ring(value, axis):
    return [value] + [shifted(value, axis, j) for j in range(1, 4)]


def to_ring(pieces, axis):
    return [pieces[0]] + [shifted(pieces[j], axis, -j) for j in range(1, 4)]


def step(grads, error, q_init):
    chip = ("x", "c", "y")
    send, squares, q = prep(grads, error, q_init.T)
    got = swap(send, "c")
    squares = exchange(squares, chip)
    *early, squares = merge(early_kernel, grads, error, got, squares, 2 * EARLY, (8,))
    early = to_ring(early, "x")
    squares = exchange(squares, "z")
    *late, shrink = merge(late_kernel, grads, error, got, squares, LATE, ())
    late = to_ring(late, "x")
    early = fold(fold_early_kernel, EARLY, *early, shrink)
    early = exchange(early, "z")
    late = exchange(fold(fold_late_kernel, LATE, *late, early), "z")
    s, pack = terms(early, late, q)

    pack = respread(exchange(pack, chip), 8)
    pack = exchange(respread(exchange(pack, "z"), SPREAD), chip)

    p_t, p_half, q = factor(pack, s)
    q = exchange(q, "z")
    parts = from_ring(q, "x")
    others = [swap(part, "c") for part in parts]
    args = (grads, error, shrink, p_half)
    outs = finish([(0, 0), (1, 0)], *args, [parts[0], others[0]])
    outs = finish([(0, 1), (0, 2), (0, 3)], *args, parts[1:], outs)
    new_error, q_t = finish([(1, 1), (1, 2), (1, 3)], *args, others[1:], outs)
    return p_t.T, q_t.T, new_error


def solution(mesh):
    finer = Mesh(
        mesh.devices.reshape(8, 4, 2, mesh.shape["tensor"]), ("z", "x", "c", "y")
    )
    replicas = ("z", "x", "c")
    return jax.shard_map(
        step,
        mesh=finer,
        in_specs=(P(replicas, None, "y"), P(replicas, None, "y"), P("y", None)),
        out_specs=(P(), P("y", None), P(replicas, None, "y")),
        check_vma=False,
    )
```

```python
import functools

import jax
import jax.numpy as jnp
from jax import lax
from jax.experimental import pallas as pl
from jax.experimental.pallas import tpu as pltpu
from jax.sharding import Mesh
from jax.sharding import PartitionSpec as P


ROWS = 160
COLS = 28672
RANK = 64
LOCAL = 7168
HALF = LOCAL // 2
QUARTER = HALF // 4
LANES = 128
BLOCKS = QUARTER // LANES
TAIL = ROWS - LANES
EARLY = 48
LATE = ROWS - EARLY
SPREAD = 32
REPLICAS = 64
EPS = 1e-06
CLIP = 0.5

f32 = jnp.float32
bf16 = jnp.bfloat16
HIGHEST = lax.Precision.HIGHEST
VMEM = pltpu.VMEM


def whole():
    return pl.BlockSpec(memory_space=VMEM)


def room(mib, flops=10**6):
    return dict(
        compiler_params=pltpu.CompilerParams(vmem_limit_bytes=mib * 2**20),
        cost_estimate=pl.CostEstimate(flops=flops, bytes_accessed=2**20, transcendentals=0),
    )


def shrink_of(squares):
    rows = jnp.sum(squares, axis=0)
    total = jnp.sum(jnp.sum(rows, axis=1, keepdims=True), axis=0, keepdims=True)
    scaled = CLIP * jnp.sqrt(f32(ROWS * COLS))
    return jnp.minimum(1.0, scaled * lax.rsqrt(total / REPLICAS + EPS))


def prep_kernel(g, e, q_all, send, squares, q, other, own, sems):
    core, x, z = (lax.axis_index(axis) for axis in ("c", "x", "z"))

    def piece(ref, core, out, sem):
        cols = pl.ds(pl.multiple_of(core * HALF, LANES), HALF)
        return pltpu.make_async_copy(ref.at[0, :, cols], out, sems.at[sem])

    top, low = slice(0, ROWS), slice(ROWS, 2 * ROWS)
    first = core * 4 * BLOCKS + x * BLOCKS + jnp.minimum(z, BLOCKS - 1)
    cols = pl.ds(pl.multiple_of(first * LANES, LANES), LANES)
    copies = [
        piece(g, 1 - core, other.at[top], 0),
        piece(g, core, own, 1),
        piece(e, 1 - core, other.at[low], 2),
        pltpu.make_async_copy(q_all.at[:, cols], q, sems.at[3]),
    ]
    out = [
        pltpu.make_async_copy(other.at[part], send.at[part], sems.at[4 + k])
        for k, part in enumerate((top, low))
    ]
    for copy in copies:
        copy.start()

    def rows_of(ref):
        def rows(i, acc):
            for lane in range(0, HALF, HALF // 4):
                block = ref[pl.ds(i * 16, 16), lane : lane + HALF // 4].astype(f32)
                block = block * block
                acc = acc + (block[:8] + block[8:])
            return acc

        return rows

    acc = jnp.zeros((8, HALF // 4), f32)
    copies[0].wait()
    out[0].start()
    acc = lax.fori_loop(0, ROWS // 16, rows_of(other), acc)
    copies[1].wait()
    copies[2].wait()
    out[1].start()
    acc = lax.fori_loop(0, ROWS // 16, rows_of(own), acc)
    part = acc[:, :LANES]
    for lane in range(LANES, HALF // 4, LANES):
        part = part + acc[:, lane : lane + LANES]
    for k in range(SPREAD):
        squares[k] = part
    copies[3].wait()
    for copy in out:
        copy.wait()


def prep(grads, error, q_t):
    hbm = pl.BlockSpec(memory_space=pltpu.HBM)
    return pl.pallas_call(
        prep_kernel,
        in_specs=[hbm, hbm, hbm],
        out_specs=[hbm, whole(), whole()],
        scratch_shapes=[
            VMEM((2 * ROWS, HALF), bf16),
            VMEM((ROWS, HALF), bf16),
            pltpu.SemaphoreType.DMA((6,)),
        ],
        out_shape=[
            jax.ShapeDtypeStruct((2 * ROWS, HALF), bf16),
            jax.ShapeDtypeStruct((SPREAD, 8, LANES), f32),
            jax.ShapeDtypeStruct((RANK, LANES), f32),
        ],
        name="prep",
        **room(58, 10**8),
    )(grads, error, q_t)


def both(g, e, got, row, core, place):
    here = pl.ds(row, 16)
    mine = pl.ds(pl.multiple_of(core * HALF + place * QUARTER, LANES), QUARTER)
    cols = pl.ds(pl.multiple_of(place * QUARTER, LANES), QUARTER)
    gradient = g[0, here, mine].astype(f32) + got[here, cols].astype(f32)
    residue = e[0, here, mine].astype(f32) + got[pl.ds(ROWS + row, 16), cols].astype(f32)
    return gradient, residue


def early_kernel(g, e, got, squares, *outs):
    outs, spread = outs[:4], outs[4]
    core, x = lax.axis_index("c"), lax.axis_index("x")
    for j, out in enumerate(outs):
        place = lax.rem(x + j, 4)

        def rows(i, carry, out=out, place=place):
            gradient, residue = both(g, e, got, i * 16, core, place)
            out[pl.ds(i * 16, 16), :] = gradient
            out[pl.ds(EARLY + i * 16, 16), :] = residue
            return carry

        lax.fori_loop(0, EARLY // 16, rows, 0)
    total = jnp.sum(squares[...], axis=0)
    for k in range(8):
        spread[k] = total


def late_kernel(g, e, got, squares, *outs):
    outs, spread = outs[:4], outs[4]
    core, x = lax.axis_index("c"), lax.axis_index("x")
    shrink = shrink_of(squares[...])
    spread[...] = jnp.broadcast_to(shrink, (8, LANES))
    for j, out in enumerate(outs):
        place = lax.rem(x + j, 4)

        def rows(i, carry, out=out, place=place):
            gradient, residue = both(g, e, got, EARLY + i * 16, core, place)
            out[pl.ds(i * 16, 16), :] = shrink * gradient + residue
            return carry

        lax.fori_loop(0, LATE // 16, rows, 0)


def merge(kernel, grads, error, got, squares, rows, spread):
    outs = [(rows, QUARTER)] * 4 + [(*spread, 8, LANES)]
    return pl.pallas_call(
        kernel,
        in_specs=[whole()] * 4,
        out_specs=[whole()] * len(outs),
        out_shape=[jax.ShapeDtypeStruct(shape, f32) for shape in outs],
        **room(16, 10**9),
    )(grads, error, got, squares)


def fold_early_kernel(a, b, c, d, shrink, out):
    shrink = shrink[0:1, 0:1]
    top, low = slice(0, EARLY), slice(EARLY, 2 * EARLY)
    for k in range(BLOCKS):
        cols = slice(k * LANES, (k + 1) * LANES)
        gradient = (a[top, cols] + c[top, cols]) + (b[top, cols] + d[top, cols])
        residue = (a[low, cols] + c[low, cols]) + (b[low, cols] + d[low, cols])
        out[k] = shrink * gradient + residue
    out[BLOCKS] = jnp.zeros((EARLY, LANES), f32)


def fold_late_kernel(a, b, c, d, after, out):
    for k in range(BLOCKS):
        cols = slice(k * LANES, (k + 1) * LANES)
        out[k] = (a[:, cols] + c[:, cols]) + (b[:, cols] + d[:, cols])
    out[BLOCKS] = jnp.zeros((LATE, LANES), f32)


def fold(kernel, rows, *args):
    return pl.pallas_call(
        kernel,
        in_specs=[whole()] * len(args),
        out_specs=whole(),
        out_shape=jax.ShapeDtypeStruct((BLOCKS + 1, rows, LANES), f32),
        **room(8, 10**8),
    )(*args)


def dot(a, b):
    return jnp.dot(a, b, precision=HIGHEST, preferred_element_type=f32)


def dot_t(a, b):
    return lax.dot_general(
        a, b, (((1,), (1,)), ((), ())), precision=HIGHEST, preferred_element_type=f32
    )


def terms_kernel(early, late, q, total, pack):
    top, low = early[0], late[0]
    for k in range(1, BLOCKS + 1):
        top = top + early[k]
        low = low + late[k]
    s = jnp.concatenate([top, low], axis=0)
    total[...] = s
    head = s[:LANES]
    tail = s[LANES:]
    tail_full = jnp.concatenate([tail, jnp.zeros((LANES - TAIL, LANES), f32)], axis=0)
    q_half = q[...].astype(bf16).astype(f32)
    left_tail = dot_t(q_half, tail_full)
    corner = dot_t(tail, tail_full)
    packed_left = left_tail[0:16]
    packed_corner = corner[0:8]
    for j in range(1, 4):
        packed_left = packed_left + pltpu.roll(left_tail[16 * j : 16 * j + 16], 32 * j, 1)
        packed_corner = packed_corner + pltpu.roll(corner[8 * j : 8 * j + 8], 32 * j, 1)
    flat = jnp.concatenate(
        [
            dot_t(q_half, head),
            dot_t(head, head),
            dot_t(tail, head),
            packed_left,
            packed_corner,
            jnp.zeros((8, LANES), f32),
        ],
        axis=0,
    )
    for k in range(SPREAD):
        pack[k] = flat[8 * k : 8 * k + 8]


def terms(early, late, q):
    return pl.pallas_call(
        terms_kernel,
        in_specs=[whole()] * 3,
        out_specs=[whole()] * 2,
        out_shape=[
            jax.ShapeDtypeStruct((ROWS, LANES), f32),
            jax.ShapeDtypeStruct((SPREAD, 8, LANES), f32),
        ],
        name="terms",
        **room(8, 10**8),
    )(early, late, q)


def across(value):
    return jnp.broadcast_to(jnp.sum(value, axis=1, keepdims=True), value.shape)


def orthonormal(a, b):
    groups = RANK // 8
    a = [a[8 * i : 8 * i + 8] for i in range(groups)]
    b = [b[8 * i : 8 * i + 8] for i in range(groups)]
    place = lax.broadcasted_iota(jnp.int32, (8, LANES), 0)
    for k in range(0, RANK, 2):
        g, r = divmod(k, 8)
        u_a, u_b = a[g][r : r + 1], b[g][r : r + 1]
        w_a, w_b = a[g][r + 1 : r + 2], b[g][r + 1 : r + 2]
        span = range(g, groups)
        by_u = [across(a[i] * u_a + b[i] * u_b) for i in span]
        by_w = [across(a[i] * w_a + b[i] * w_b) for i in span]
        uu, uw = by_u[0][r : r + 1], by_u[0][r + 1 : r + 2]
        ww = by_w[0][r + 1 : r + 2]
        over_u = 1.0 / (uu + EPS)
        along = uw * over_u
        rest = uw - along * uu
        over_w = 1.0 / (jnp.maximum(ww - along * (uw + rest), 0.0) + EPS)
        w_a = w_a - along * u_a
        w_b = w_b - along * u_b
        for i in span:
            coeff_u = by_u[i - g] * over_u
            coeff_w = (by_w[i - g] - along * by_u[i - g] - coeff_u * rest) * over_w
            if i == g:
                coeff_u = jnp.where(place > r, coeff_u, 0.0)
                coeff_w = jnp.where(place > r + 1, coeff_w, 0.0)
            a[i] = a[i] - coeff_u * u_a - coeff_w * w_a
            b[i] = b[i] - coeff_u * u_b - coeff_w * w_b
    for i in range(groups):
        scale = lax.rsqrt(across(a[i] * a[i] + b[i] * b[i]) + EPS)
        a[i] = a[i] * scale
        b[i] = b[i] * scale
    return jnp.concatenate(a, axis=0), jnp.concatenate(b, axis=0)


def factor_kernel(pack, s, p_t, p_half, q):
    lane = lax.broadcasted_iota(jnp.int32, (1, LANES), 1)
    keep = lane < TAIL

    def unpack(rows):
        parts = [jnp.where(keep, rows, 0.0)]
        for j in range(1, 4):
            parts.append(jnp.where(keep, pltpu.roll(rows, LANES - 32 * j, 1), 0.0))
        return jnp.concatenate(parts, axis=0)

    flat = jnp.concatenate([pack[k] for k in range(SPREAD)], axis=0)
    empty = jnp.zeros((LANES - TAIL, LANES), f32)
    first_a = flat[0:64]
    gram = flat[64 : 64 + LANES]
    gram_side = jnp.concatenate([flat[64 + LANES : 64 + ROWS], empty], axis=0)
    first_b = unpack(flat[224:240])
    gram_corner = jnp.concatenate([unpack(flat[240:248]), empty], axis=0)

    a, b = orthonormal(first_a, first_b)
    a = a.astype(bf16).astype(f32)
    b = b.astype(bf16).astype(f32)
    second_a = (dot(a, gram) + dot(b, gram_side)) * (1.0 / REPLICAS)
    second_b = (dot_t(a, gram_side) + dot(b, gram_corner)) * (1.0 / REPLICAS)
    a, b = orthonormal(second_a, second_b)
    p_t[:, 0:LANES] = a
    p_t[:, LANES:ROWS] = b[:, 0:TAIL]
    a = a.astype(bf16).astype(f32)
    b = b.astype(bf16).astype(f32)
    p_half[:, 0:LANES] = a.astype(bf16)
    p_half[:, LANES:ROWS] = b[:, 0:TAIL].astype(bf16)
    tail_full = jnp.concatenate([s[LANES:ROWS], empty], axis=0)
    columns = ((dot(a, s[0:LANES]) + dot(b, tail_full)) * (1.0 / REPLICAS)).astype(q.dtype)
    for k in range(8):
        q[k] = columns


def factor(pack, s):
    return pl.pallas_call(
        factor_kernel,
        in_specs=[whole()] * 2,
        out_specs=[whole()] * 3,
        out_shape=[
            jax.ShapeDtypeStruct((RANK, ROWS), f32),
            jax.ShapeDtypeStruct((RANK, ROWS), bf16),
            jax.ShapeDtypeStruct((8, RANK, LANES), bf16),
        ],
        name="factor",
        **room(8, 100000000),
    )(pack, s)


def finish_kernel(which, g, e, shrink, p_half, *refs):
    n = len(which)
    parts = refs[:n]
    out, q_t, new, right_part, sems = refs[-5:]
    shrink = shrink[0:1, 0:1]
    core, x = lax.axis_index("c"), lax.axis_index("x")
    left = p_half[...].astype(f32).T.astype(bf16)
    copies = []
    for k, (other, ahead) in enumerate(which):
        place = (1 - core if other else core) * 4 + lax.rem(x + ahead, 4)
        first = place * QUARTER
        for block in range(BLOCKS):
            cols = slice(block * LANES, (block + 1) * LANES)
            here = pl.ds(pl.multiple_of(first + block * LANES, LANES), LANES)
            q = parts[k][block]
            approx = jnp.dot(left, q, preferred_element_type=f32)
            merged = shrink * g[0, :, here].astype(f32) + e[0, :, here].astype(f32)
            new[k, :, cols] = merged - approx
            right_part[k, :, cols] = q.astype(f32)
        cols = pl.ds(pl.multiple_of(first, LANES), QUARTER)
        for j, rows in enumerate((slice(0, ROWS // 2), slice(ROWS // 2, ROWS))):
            copies.append(
                pltpu.make_async_copy(new.at[k, rows], out.at[0, rows, cols], sems.at[3 * k + j])
            )
        copies.append(pltpu.make_async_copy(right_part.at[k], q_t.at[:, cols], sems.at[3 * k + 2]))
        for copy in copies[-3:]:
            copy.start()
    for copy in copies:
        copy.wait()


def finish(which, grads, error, shrink, p_half, parts, before=()):
    n = len(parts)
    hbm = pl.BlockSpec(memory_space=pltpu.HBM)
    return pl.pallas_call(
        functools.partial(finish_kernel, which),
        in_specs=[whole()] * (4 + n) + [hbm] * len(before),
        out_specs=[hbm, hbm],
        scratch_shapes=[
            VMEM((n, ROWS, QUARTER), f32),
            VMEM((n, RANK, QUARTER), f32),
            pltpu.SemaphoreType.DMA((3 * n,)),
        ],
        out_shape=[
            jax.ShapeDtypeStruct((1, ROWS, LOCAL), f32),
            jax.ShapeDtypeStruct((RANK, LOCAL), f32),
        ],
        input_output_aliases={4 + n: 0, 5 + n: 1} if before else {},
        name="finish",
        **room(12, 10**9),
    )(grads, error, shrink, p_half, *parts, *before)


def respread_kernel(blocks, out):
    total = blocks[0]
    for k in range(1, blocks.shape[0]):
        total = total + blocks[k]
    for k in range(out.shape[0]):
        out[k] = total


def respread(blocks, n):
    return pl.pallas_call(
        respread_kernel,
        in_specs=[whole()],
        out_specs=whole(),
        out_shape=jax.ShapeDtypeStruct((n, *blocks.shape[1:]), f32),
        name="respread",
        **room(4, 1000000),
    )(blocks)


def shifted(value, axis, by):
    n = lax.axis_size(axis)
    return lax.ppermute(value, axis, [(i, (i - by) % n) for i in range(n)])


def swap(value, axis):
    return lax.ppermute(value, axis, [(0, 1), (1, 0)])


def exchange(blocks, axis):
    return lax.all_to_all(blocks, axis, 0, 0, tiled=True)


def from_ring(value, axis):
    return [value] + [shifted(value, axis, j) for j in range(1, 4)]


def to_ring(pieces, axis):
    return [pieces[0]] + [shifted(pieces[j], axis, -j) for j in range(1, 4)]


def step(grads, error, q_init):
    chip = ("x", "c", "y")
    send, squares, q = prep(grads, error, q_init.T)
    got = swap(send, "c")
    squares = exchange(squares, chip)
    *early, squares = merge(early_kernel, grads, error, got, squares, 2 * EARLY, (8,))
    early = to_ring(early, "x")
    squares = exchange(squares, "z")
    *late, shrink = merge(late_kernel, grads, error, got, squares, LATE, ())
    late = to_ring(late, "x")
    early = fold(fold_early_kernel, EARLY, *early, shrink)
    early = exchange(early, "z")
    late = exchange(fold(fold_late_kernel, LATE, *late, early), "z")
    s, pack = terms(early, late, q)

    pack = respread(exchange(pack, chip), 8)
    pack = exchange(respread(exchange(pack, "z"), SPREAD), chip)

    p_t, p_half, q = factor(pack, s)
    q = exchange(q, "z")
    parts = from_ring(q, "x")
    others = [swap(part, "c") for part in parts]
    args = (grads, error, shrink, p_half)
    outs = finish([(0, 0), (1, 0)], *args, [parts[0], others[0]])
    outs = finish([(0, 1), (0, 2), (0, 3)], *args, parts[1:], outs)
    new_error, q_t = finish([(1, 1), (1, 2), (1, 3)], *args, others[1:], outs)
    return p_t.T, q_t.T, new_error


def solution(mesh):
    finer = Mesh(
        mesh.devices.reshape(8, 4, 2, mesh.shape["tensor"]), ("z", "x", "c", "y")
    )
    replicas = ("z", "x", "c")
    return jax.shard_map(
        step,
        mesh=finer,
        in_specs=(P(replicas, None, "y"), P(replicas, None, "y"), P("y", None)),
        out_specs=(P(), P("y", None), P(replicas, None, "y")),
        check_vma=False,
    )
```
